128 devices in a mesh: gx: 2 (over z_lo), gy: 2 (over core), gz: 32 (over z_hi, y, x).
Axes of the slice: x: 4, y: 4, z: 4 (z_hi: 2, z_lo: 2; z = z_hi * 2 + z_lo), core: 2. Of those that a mesh axis runs over, the one named last changes fastest.
Arguments:
- state_re: float32 [134217728], P(('gx', 'gy', 'gz')), may hold values from -6 to 6
- state_im: float32 [134217728], P(('gx', 'gy', 'gz')), may hold values from -6 to 6
Outputs:
- out_re: float32 [134217728], P(('gx', 'gy', 'gz'))
- out_im: float32 [134217728], P(('gx', 'gy', 'gz'))
- probability: float32 [134217728], P(('gx', 'gy', 'gz'))
The draws below stay inside these ranges and needn't reach their ends.
All inputs are finite; a program needn't handle non-finite values.
Results may differ from the reference program's by a relative error of at most 0.000071.
Values sent between devices are 32-bit elements; how exact they have to be, the bound alone decides.
A program may use at most 128 MiB of HBM per device.

```python
import jax
import jax.numpy as jnp

AMPS = 1048576
NSTATE = 134217728
DEVICES = 128


def levels(key, dims, shards, smallest, top_value):
    factor_of, own = 1.0, jax.random.fold_in(key, 6)
    for dim, blocks in shards:
        draws = jnp.exp(jax.random.uniform(jax.random.fold_in(own, dim), (blocks,), jnp.float32, smallest / len(shards), top_value / len(shards)))
        factor_of = factor_of * jnp.repeat(draws, dims[dim] // blocks).reshape([-1 if axis == dim else 1 for axis in range(len(dims))])
    return factor_of


def gaussian(key, shape, deviation, reach, pieces=(), dtype=jnp.bfloat16):
    factor_of = levels(key, shape, pieces, -0.22, 0.18) if pieces else 1.0
    drawn = jax.random.normal(key, shape, jnp.float32) * deviation * factor_of
    return jnp.minimum(jnp.maximum(drawn, -reach), reach).astype(dtype)


def setup_inputs(seed: int = 0) -> dict:
    arg_keys = jax.random.split(jax.random.key(seed), 3)
    state_re = gaussian(arg_keys[0], (NSTATE,), 1.0, 6.0, ((0, 128),), jnp.float32)
    state_im = gaussian(arg_keys[1], (NSTATE,), 1.0, 6.0, ((0, 128),), jnp.float32)
    return dict(state_re=state_re, state_im=state_im)


def reverse_bits(values, nbits, total):
    shaped = values.reshape((2,) * nbits)
    return jnp.transpose(shaped, tuple(range(nbits - 1, -1, -1))).reshape(total)


def reference(state_re, state_im):
    total = AMPS * DEVICES
    nbits = total.bit_length() - 1
    state = state_re + 1j * state_im
    spectrum = jnp.fft.ifft(state, norm="ortho")
    out_re = reverse_bits(jnp.real(spectrum), nbits, total).astype(jnp.float32)
    out_im = reverse_bits(jnp.imag(spectrum), nbits, total).astype(jnp.float32)
    probability = out_re * out_re + out_im * out_im
    return out_re, out_im, probability
```

```python
import functools

import jax
import jax.numpy as jnp
import numpy as np
from jax import lax
from jax.experimental import pallas as pl
from jax.experimental.pallas import tpu as pltpu
from jax.sharding import PartitionSpec as P

MESH = pl.DeviceIdType.MESH
AXES = ("gx", "gy", "gz")
N, B, C = 128, 64, 128
CHUNKS = 8
ROWS = B // CHUNKS
LOG_TOTAL = 27


def rev(values, bits):
    values = np.asarray(values)
    return sum(((values >> i) & 1) << (bits - 1 - i) for i in range(bits))


def wave(product, bits):
    angle = 2.0 * np.pi * (product % (1 << bits)) / (1 << bits)
    return np.cos(angle), np.sin(angle)


def split(matrix):
    high = jnp.asarray(matrix, jnp.float32).astype(jnp.bfloat16)
    low = (jnp.asarray(matrix, jnp.float32) - high.astype(jnp.float32)).astype(jnp.bfloat16)
    return high, low


def np_split(matrix):
    high = np.asarray(matrix, np.float32).astype(jnp.bfloat16)
    low = (np.asarray(matrix, np.float64) - high.astype(np.float64)).astype(jnp.bfloat16)
    return high, low


def tables():
    i = np.arange(N)
    k = rev(i, 7)
    wr, wi = wave(np.outer(k, i), 7)
    mix = np.block([[wr, -wi], [wi, wr]])
    both = lambda pair: np.concatenate(pair, axis=0).astype(np.float32)
    owner = both(wave(np.outer(k, i), 14))
    low_in = both(wave(np.outer(k, i), 27))
    low_out = both(wave(np.outer(k, i), 20))
    e = np.arange(8)
    steps = np.zeros((2 * N, C), np.float32)
    for at, bits in ((0, 20), (32, 13)):
        steps[:, at : at + 8] = both(wave(np.outer(k, e), bits))
        steps[:, at + 8 : at + 16] = both(wave(np.outer(k, 8 * e), bits))
    j = np.arange(B)
    kb = rev(j, 6)
    br, bi = wave(np.outer(kb, j), 6)
    b_hi, b_lo = np_split(np.block([[br, -bi], [bi, br]]))
    inner = np.concatenate([b_hi, b_hi, b_lo], axis=1)
    turn = both(wave(np.outer(kb, i), 13))
    cr, ci = wave(np.outer(i, k), 7)
    scale = 2.0 ** (-LOG_TOTAL / 2)
    last = np.block([[cr, ci], [-ci, cr]]) * scale
    return dict(
        mix=np_split(mix), owner=owner, low_in=low_in, low_out=low_out, steps=steps,
        inner=inner, turn=turn, last=np_split(last),
    )


def place():
    gx, gy, gz = (lax.axis_index(a) for a in AXES)
    return gz % 4, (gz // 4) % 4, (gz // 16) * 2 + gx, gy


def halves(x):
    high = x.astype(jnp.bfloat16)
    return high, (x - high.astype(jnp.float32)).astype(jnp.bfloat16)


def dot(a, b):
    return jnp.dot(a, b, preferred_element_type=jnp.float32)


def exchange_kernel(
    in_re, in_im, mix_hi, mix_lo, owner, low_in, low_out, steps, out,
    got, sent, back, done, w_hi, w_lo, own_t, in_t, out_t, step_t, in_fine, in_coarse, out_fine, out_coarse,
    send_sem, own_sem, table_sem, first_sem, second_sem, write_sem,
):
    x, y, z, core = place()
    me = (z % 2) * 64 + core * 32 + (z // 2) * 16 + y * 4 + x

    def partner(step):
        px = (x + step) % 4
        py = (y + step // 4) % 4
        pz = (z + step // 16) % 4
        pc = (core + step // 64) % 2
        gx, gz = pz % 2, (pz // 2) * 16 + py * 4 + px
        return gx * 64 + pc * 32 + gz, (gx, pc, gz)

    def push(src, dst, sem, device):
        pltpu.make_async_remote_copy(src, dst, send_sem, sem, device_id=device, device_id_type=MESH).start()

    def leg_one(i, _):
        chunk, step = i // 127, i % 127 + 1
        rows = pl.ds(chunk * ROWS, ROWS)
        d, device = partner(step)
        push(in_re.at[d, rows], got.at[rows, me], first_sem.at[chunk], device)
        push(in_im.at[d, rows], got.at[rows, N + me], first_sem.at[chunk], device)
        return 0

    own = [pltpu.make_async_copy(src.at[me], got.at[:, at + me], own_sem) for src, at in ((in_re, 0), (in_im, N))]
    loads = [
        pltpu.make_async_copy(src, dst, table_sem.at[n])
        for n, (src, dst) in enumerate(
            ((mix_hi, w_hi), (mix_lo, w_lo), (owner, own_t), (low_in, in_t), (low_out, out_t), (steps, step_t))
        )
    ]
    lax.fori_loop(0, 127 * CHUNKS, leg_one, 0)
    for copy in own + loads:
        copy.start()
    for copy in loads:
        copy.wait()

    def spread(column):
        return jnp.broadcast_to(column, (N, C))

    lane = lax.broadcasted_iota(jnp.int32, (N, C), 1)
    mine = [jnp.sum(jnp.where(lane == me, own_t[at : at + N], 0.0), axis=1, keepdims=True) for at in (0, N)]
    for low, fine, coarse, at, extra in ((in_t, in_fine, in_coarse, 0, mine), (out_t, out_fine, out_coarse, 32, None)):
        lr, li = low[:N], low[N:]
        if extra is not None:
            er, ei = spread(extra[0]), spread(extra[1])
            lr, li = lr * er - li * ei, lr * ei + li * er
        for e in range(8):
            sr, si = spread(step_t[:N, at + e : at + e + 1]), spread(step_t[N:, at + e : at + e + 1])
            fine[e, :N] = lr * sr - li * si
            fine[e, N:] = lr * si + li * sr
            coarse[e, :N] = spread(step_t[:N, at + 8 + e : at + 9 + e])
            coarse[e, N:] = spread(step_t[N:, at + 8 + e : at + 9 + e])

    def transform(src, dst, chunk, fine, coarse):
        def pair(q, _):
            b = chunk * ROWS + 2 * q
            hi, lo = halves(jnp.concatenate([src[b], src[b + 1]], axis=1))
            whi = w_hi[...]
            mixed = dot(whi, hi) + dot(whi, lo) + dot(w_lo[...], hi)
            for h in range(2):
                low, high = (b + h) % 8, (b + h) // 8
                fr, fi, cr, ci = fine[low, :N], fine[low, N:], coarse[high, :N], coarse[high, N:]
                tr, ti = fr * cr - fi * ci, fr * ci + fi * cr
                mr, mi = mixed[:N, h * C : (h + 1) * C], mixed[N:, h * C : (h + 1) * C]
                dst[b + h, :N] = mr * tr - mi * ti
                dst[b + h, N:] = mr * ti + mi * tr
            return 0

        lax.fori_loop(0, ROWS // 2, pair, 0)

    for copy in own:
        copy.wait()

    def there(chunk, _):
        rows = pl.ds(chunk * ROWS, ROWS)
        taken = got.at[rows, pl.ds(0, 254)]
        pltpu.make_async_copy(taken, taken, first_sem.at[chunk]).wait()
        transform(got, sent, chunk, in_fine, in_coarse)

        def leg_two(i, _):
            d, device = partner(i + 1)
            push(sent.at[rows, d], back.at[rows, me], second_sem.at[chunk], device)
            push(sent.at[rows, N + d], back.at[rows, N + me], second_sem.at[chunk], device)
            return 0

        lax.fori_loop(0, 127, leg_two, 0)
        for at in (0, N):
            back[rows, pl.ds(at + me, 1), :] = sent[rows, pl.ds(at + me, 1), :]
        return 0

    lax.fori_loop(0, CHUNKS, there, 0)

    def home(chunk, _):
        rows = pl.ds(chunk * ROWS, ROWS)
        taken = back.at[rows, pl.ds(0, 254)]
        pltpu.make_async_copy(taken, taken, second_sem.at[chunk]).wait()
        transform(back, done, chunk, out_fine, out_coarse)

        def write(r, _):
            b = chunk * ROWS + r
            pltpu.make_async_copy(done.at[b], out.at[:, b], write_sem).start()
            return 0

        lax.fori_loop(0, ROWS, write, 0)
        return 0

    lax.fori_loop(0, CHUNKS, home, 0)
    pltpu.make_async_copy(done, done, write_sem).wait()
    for _ in range(4):
        moved = got.at[:, pl.ds(0, 127)]
        pltpu.make_async_copy(moved, moved, send_sem).wait()


def finish_kernel(z, inner, turn, last_hi, last_lo, out_re, out_im, prob, hi_s, lo_s):
    count = z.shape[1]
    mat = inner[...]
    vr, vi = turn[:B], turn[B:]
    for q in range(count // 2):
        both = [jnp.concatenate([z[part, 2 * q], z[part, 2 * q + 1]], axis=1) for part in range(2)]
        hi, lo = halves(jnp.concatenate(both, axis=0))
        mixed = dot(mat, jnp.concatenate([hi, lo, hi], axis=0))
        for h in range(2):
            mr, mi = mixed[:B, h * C : (h + 1) * C], mixed[B:, h * C : (h + 1) * C]
            at = (2 * q + h) * B
            for value, lanes in ((mr * vr - mi * vi, slice(0, C)), (mr * vi + mi * vr, slice(C, 2 * C))):
                high, low = halves(value)
                hi_s[at : at + B, lanes] = high
                lo_s[at : at + B, lanes] = low
    result = dot(hi_s[...], last_hi[...]) + dot(lo_s[...], last_hi[...]) + dot(hi_s[...], last_lo[...])
    re = result[:, :C]
    im = result[:, C:]
    out_re[...] = re.reshape(out_re.shape)
    out_im[...] = im.reshape(out_im.shape)
    prob[...] = (re * re + im * im).reshape(prob.shape)


def solution(mesh):
    t = tables()
    f32, bf16 = jnp.float32, jnp.bfloat16
    anywhere = pl.BlockSpec(memory_space=pl.ANY)
    cube = pltpu.VMEM((B, 2 * N, C), f32)
    table = pltpu.VMEM((2 * N, C), f32)
    fan = pltpu.VMEM((8, 2 * N, C), f32)
    dma = pltpu.SemaphoreType.DMA

    exchange = pl.pallas_call(
        exchange_kernel,
        out_shape=jax.ShapeDtypeStruct((2 * N, B, C), f32),
        in_specs=[anywhere] * 8,
        out_specs=anywhere,
        scratch_shapes=[
            cube, cube, cube, cube,
            pltpu.VMEM((2 * N, 2 * N), bf16), pltpu.VMEM((2 * N, 2 * N), bf16),
            table, table, table, table, fan, fan, fan, fan,
            dma, dma, dma((6,)), dma((CHUNKS,)), dma((CHUNKS,)), dma,
        ],
        compiler_params=pltpu.CompilerParams(has_side_effects=True, vmem_limit_bytes=60 << 20),
    )
    block = 8
    whole = lambda shape: pl.BlockSpec(shape, lambda i: (0,) * len(shape))
    finish = pl.pallas_call(
        finish_kernel,
        grid=(N // block,),
        out_shape=[jax.ShapeDtypeStruct((N, B, C), f32)] * 3,
        in_specs=[
            pl.BlockSpec((2, block, B, C), lambda i: (0, i, 0, 0)),
            whole((2 * B, 6 * B)), whole((2 * B, C)), whole((2 * C, 2 * C)), whole((2 * C, 2 * C)),
        ],
        out_specs=[pl.BlockSpec((block, B, C), lambda i: (i, 0, 0))] * 3,
        scratch_shapes=[pltpu.VMEM((block * B, 2 * C), bf16)] * 2,
        compiler_params=pltpu.CompilerParams(dimension_semantics=("arbitrary",), vmem_limit_bytes=40 << 20),
    )

    def on_device(state_re, state_im):
        cut = (N, B, C)
        z = exchange(
            state_re.reshape(cut), state_im.reshape(cut), *map(jnp.asarray, t["mix"]),
            *(jnp.asarray(t[name]) for name in ("owner", "low_in", "low_out", "steps")),
        )
        outs = finish(z.reshape(2, N, B, C), jnp.asarray(t["inner"]), jnp.asarray(t["turn"]), *map(jnp.asarray, t["last"]))
        return tuple(o.reshape(N * B * C) for o in outs)

    spec = P(AXES)
    return jax.shard_map(on_device, mesh=mesh, in_specs=(spec, spec), out_specs=(spec,) * 3, check_vma=False)
```

```python
import functools

import jax
import jax.numpy as jnp
import numpy as np
from jax import lax
from jax.experimental import pallas as pl
from jax.experimental.pallas import tpu as pltpu
from jax.sharding import PartitionSpec as P

MESH = pl.DeviceIdType.MESH
AXES = ("gx", "gy", "gz")
N, B, C = 128, 64, 128
CHUNKS = 8
ROWS = B // CHUNKS
LOG_TOTAL = 27


def rev(values, bits):
    values = np.asarray(values)
    return sum(((values >> i) & 1) << (bits - 1 - i) for i in range(bits))


def wave(product, bits):
    angle = 2.0 * np.pi * (product % (1 << bits)) / (1 << bits)
    return np.cos(angle), np.sin(angle)


def np_split(matrix):
    high = np.asarray(matrix, np.float32).astype(jnp.bfloat16)
    low = (np.asarray(matrix, np.float64) - high.astype(np.float64)).astype(jnp.bfloat16)
    return high, low


def tables():
    i = np.arange(N)
    k = rev(i, 7)
    wr, wi = wave(np.outer(k, i), 7)
    mix = np.block([[wr, -wi], [wi, wr]])
    both = lambda pair: np.concatenate(pair, axis=0).astype(np.float32)
    owner = both(wave(np.outer(k, i), 14))
    low_in = both(wave(np.outer(k, i), 27))
    low_out = both(wave(np.outer(k, i), 20))
    e = np.arange(8)
    steps = np.zeros((2 * N, C), np.float32)
    for at, bits in ((0, 20), (32, 13)):
        steps[:, at : at + 8] = both(wave(np.outer(k, e), bits))
        steps[:, at + 8 : at + 16] = both(wave(np.outer(k, 8 * e), bits))
    j = np.arange(8)
    middle = [both(wave(np.outer(j, 128 * chunk + i), 13)) for chunk in range(CHUNKS)]
    turn = both(wave(np.outer(j, i), 10))
    cr, ci = wave(np.outer(i, k), 7)
    scale = 2.0 ** (-LOG_TOTAL / 2)
    last = np.block([[cr, ci], [-ci, cr]]) * scale
    return dict(
        mix=np_split(mix), owner=owner, low_in=low_in, low_out=low_out, steps=steps,
        middle=np.stack(middle), turn=turn, last=np_split(last),
    )


def place():
    gx, gy, gz = (lax.axis_index(a) for a in AXES)
    return gz % 4, (gz // 4) % 4, (gz // 16) * 2 + gx, gy


def halves(x):
    high = x.astype(jnp.bfloat16)
    return high, (x - high.astype(jnp.float32)).astype(jnp.bfloat16)


def dot(a, b):
    return jnp.dot(a, b, preferred_element_type=jnp.float32)


def eight(v):
    def add(p, q):
        return p[0] + q[0], p[1] + q[1]

    def sub(p, q):
        return p[0] - q[0], p[1] - q[1]

    def turn(p):
        return -p[1], p[0]

    def four(p):
        s, d, t, u = add(p[0], p[2]), sub(p[0], p[2]), add(p[1], p[3]), turn(sub(p[1], p[3]))
        return add(s, t), add(d, u), sub(s, t), sub(d, u)

    root = 0.5**0.5
    even, odd = four(v[0::2]), four(v[1::2])
    r, i = odd[1]
    one = ((r - i) * root, (r + i) * root)
    r, i = odd[3]
    three = ((r + i) * -root, (r - i) * root)
    odd = (odd[0], one, turn(odd[2]), three)
    return [add(even[k], odd[k]) for k in range(4)] + [sub(even[k], odd[k]) for k in range(4)]


def times(p, q):
    return p[0] * q[0] - p[1] * q[1], p[0] * q[1] + p[1] * q[0]


def exchange_kernel(
    in_re, in_im, mix_hi, mix_lo, owner, low_in, low_out, steps, middle, out,
    got, sent, back, work, w_hi, w_lo, own_t, in_t, out_t, step_t, middle_t, in_fine, in_coarse, out_fine, out_coarse,
    send_sem, own_sem, table_sem, first_sem, second_sem,
):
    x, y, z, core = place()
    me = (z % 2) * 64 + core * 32 + (z // 2) * 16 + y * 4 + x

    def partner(step):
        px = (x + step) % 4
        py = (y + step // 4) % 4
        pz = (z + step // 16) % 4
        pc = (core + step // 64) % 2
        gx, gz = pz % 2, (pz // 2) * 16 + py * 4 + px
        return gx * 64 + pc * 32 + gz, (gx, pc, gz)

    def push(src, dst, sem, device):
        pltpu.make_async_remote_copy(src, dst, send_sem, sem, device_id=device, device_id_type=MESH).start()

    def leg_one(i, _):
        chunk, step = i // 127, i % 127 + 1
        d, device = partner(step)
        push(in_re.at[d, :, chunk], got.at[chunk, :, me], first_sem.at[chunk], device)
        push(in_im.at[d, :, chunk], got.at[chunk, :, N + me], first_sem.at[chunk], device)
        return 0

    own = [
        pltpu.make_async_copy(src.at[me, :, chunk], got.at[chunk, :, at + me], own_sem)
        for src, at in ((in_re, 0), (in_im, N))
        for chunk in range(CHUNKS)
    ]
    loads = [
        pltpu.make_async_copy(src, dst, table_sem.at[n])
        for n, (src, dst) in enumerate(
            (
                (mix_hi, w_hi), (mix_lo, w_lo), (owner, own_t), (low_in, in_t), (low_out, out_t), (steps, step_t),
                (middle, middle_t),
            )
        )
    ]
    lax.fori_loop(0, 127 * CHUNKS, leg_one, 0)
    for copy in own + loads:
        copy.start()
    for copy in loads:
        copy.wait()

    def spread(column):
        return jnp.broadcast_to(column, (N, C))

    lane = lax.broadcasted_iota(jnp.int32, (N, C), 1)
    mine = [jnp.sum(jnp.where(lane == me, own_t[at : at + N], 0.0), axis=1, keepdims=True) for at in (0, N)]
    for low, fine, coarse, at, extra in ((in_t, in_fine, in_coarse, 0, mine), (out_t, out_fine, out_coarse, 32, None)):
        value = low[:N], low[N:]
        if extra is not None:
            value = times(value, (spread(extra[0]), spread(extra[1])))
        for e in range(8):
            step = spread(step_t[:N, at + e : at + e + 1]), spread(step_t[N:, at + e : at + e + 1])
            fine[e, :N], fine[e, N:] = times(value, step)
            coarse[e, :N] = spread(step_t[:N, at + 8 + e : at + 9 + e])
            coarse[e, N:] = spread(step_t[N:, at + 8 + e : at + 9 + e])

    def transform(src, dst, chunk, fine, coarse):
        def pair(q, _):
            hi, lo = halves(jnp.concatenate([src[2 * q], src[2 * q + 1]], axis=1))
            whi = w_hi[...]
            mixed = dot(whi, hi) + dot(whi, lo) + dot(w_lo[...], hi)
            for h in range(2):
                b = 2 * q + h
                turn = times((fine[chunk, :N], fine[chunk, N:]), (coarse[b, :N], coarse[b, N:]))
                part = mixed[:, h * C : (h + 1) * C]
                dst[b, :N], dst[b, N:] = times((part[:N], part[N:]), turn)
            return 0

        lax.fori_loop(0, ROWS // 2, pair, 0)

    for _ in range(2):
        pltpu.make_async_copy(in_re.at[0], in_re.at[0], own_sem).wait()

    def there(chunk, _):
        taken = got.at[chunk, :, pl.ds(0, 254)]
        pltpu.make_async_copy(taken, taken, first_sem.at[chunk]).wait()
        transform(got.at[chunk], sent.at[chunk], chunk, in_fine, in_coarse)

        def leg_two(i, _):
            d, device = partner(i + 1)
            push(sent.at[chunk, :, d], back.at[chunk, :, me], second_sem.at[chunk], device)
            push(sent.at[chunk, :, N + d], back.at[chunk, :, N + me], second_sem.at[chunk], device)
            return 0

        lax.fori_loop(0, 127, leg_two, 0)
        for at in (0, N):
            back[chunk, :, pl.ds(at + me, 1), :] = sent[chunk, :, pl.ds(at + me, 1), :]
        return 0

    lax.fori_loop(0, CHUNKS, there, 0)

    def home(chunk, _):
        taken = back.at[chunk, :, pl.ds(0, 254)]
        pltpu.make_async_copy(taken, taken, second_sem.at[chunk]).wait()
        transform(back.at[chunk], work, chunk, out_fine, out_coarse)

        def butterfly(r, _):
            re, im = pl.ds(pl.multiple_of(r * 8, 8), 8), pl.ds(pl.multiple_of(N + r * 8, 8), 8)
            for k, value in enumerate(eight([(work[b, re], work[b, im]) for b in range(8)])):
                turn = middle_t[chunk, k : k + 1], middle_t[chunk, 8 + k : 9 + k]
                out[chunk, k, re], out[chunk, k, im] = times(value, turn)
            return 0

        lax.fori_loop(0, N // 8, butterfly, 0)
        return 0

    lax.fori_loop(0, CHUNKS, home, 0)
    for _ in range(4):
        for chunk in range(CHUNKS):
            moved = got.at[chunk, :, pl.ds(0, 127)]
            pltpu.make_async_copy(moved, moved, send_sem).wait()


GROUP = 32


def finish_kernel(z, turn, last_hi, last_lo, out_re, out_im, prob, stage, out_sem):
    outs = (out_re, out_im, prob)

    def block(k, slot):
        @pl.when(k >= 2)
        def _():
            pltpu.make_async_copy(stage.at[slot], stage.at[slot], out_sem.at[slot]).wait()

        for g in range(N // GROUP):
            re, im = slice(g * GROUP, (g + 1) * GROUP), slice(N + g * GROUP, N + (g + 1) * GROUP)
            high, low = [], []
            for n, value in enumerate(eight([(z[b, k, re], z[b, k, im]) for b in range(8)])):
                parts = [halves(v) for v in times(value, (turn[n : n + 1], turn[8 + n : 9 + n]))]
                high.append(jnp.concatenate([p[0] for p in parts], axis=1))
                low.append(jnp.concatenate([p[1] for p in parts], axis=1))
            high, low = jnp.concatenate(high, axis=0), jnp.concatenate(low, axis=0)
            result = dot(high, last_hi[...]) + dot(low, last_hi[...]) + dot(high, last_lo[...])
            for n in range(8):
                r, i = result[n * GROUP : (n + 1) * GROUP, :C], result[n * GROUP : (n + 1) * GROUP, C:]
                for o, value in enumerate((r, i, r * r + i * i)):
                    stage[slot, o, n, re] = value
        first = (k % 2) * 32 + (k // 2 % 2) * 16 + (k // 4) * 8
        for o, ref in enumerate(outs):
            for n in range(8):
                pltpu.make_async_copy(stage.at[slot, o, n], ref.at[:, first + int(rev(n, 3))], out_sem.at[slot]).start()

    def two(i, _):
        for slot in range(2):
            block(2 * i + slot, slot)
        return 0

    lax.fori_loop(0, 4, two, 0)
    for slot in range(2):
        pltpu.make_async_copy(stage.at[slot], stage.at[slot], out_sem.at[slot]).wait()


def solution(mesh):
    t = tables()
    f32, bf16 = jnp.float32, jnp.bfloat16
    anywhere, near = pl.BlockSpec(memory_space=pl.ANY), pl.BlockSpec(memory_space=pltpu.VMEM)
    far = pl.BlockSpec(memory_space=pltpu.HBM)
    cube = pltpu.VMEM((CHUNKS, ROWS, 2 * N, C), f32)
    table = pltpu.VMEM((2 * N, C), f32)
    fan = pltpu.VMEM((8, 2 * N, C), f32)
    dma = pltpu.SemaphoreType.DMA

    exchange = pl.pallas_call(
        exchange_kernel,
        out_shape=cube,
        in_specs=[far] * 2 + [anywhere] * 7,
        out_specs=near,
        scratch_shapes=[
            cube, cube, cube, fan,
            pltpu.VMEM((2 * N, 2 * N), bf16), pltpu.VMEM((2 * N, 2 * N), bf16),
            table, table, table, table, pltpu.VMEM((CHUNKS, 16, C), f32), fan, fan, fan, fan,
            dma, dma, dma((7,)), dma((CHUNKS,)), dma((CHUNKS,)),
        ],
        compiler_params=pltpu.CompilerParams(has_side_effects=True, vmem_limit_bytes=48 << 20),
    )
    finish = pl.pallas_call(
        finish_kernel,
        out_shape=[jax.ShapeDtypeStruct((N, B, C), f32)] * 3,
        in_specs=[near] * 4,
        out_specs=[far] * 3,
        scratch_shapes=[pltpu.VMEM((2, 3, 8, N, C), f32), dma((2,))],
        compiler_params=pltpu.CompilerParams(vmem_limit_bytes=24 << 20),
    )

    def on_device(state_re, state_im):
        cut = (N, 8, 8, C)
        states = [pltpu.with_memory_space_constraint(s.reshape(cut), pltpu.HBM) for s in (state_re, state_im)]
        names = ("owner", "low_in", "low_out", "steps", "middle")
        z = exchange(*states, *map(jnp.asarray, t["mix"]), *(jnp.asarray(t[name]) for name in names))
        z = pltpu.with_memory_space_constraint(z, pltpu.VMEM)
        outs = finish(z, jnp.asarray(t["turn"]), *map(jnp.asarray, t["last"]))
        return tuple(o.reshape(N * B * C) for o in outs)

    spec = P(AXES)
    return jax.shard_map(on_device, mesh=mesh, in_specs=(spec, spec), out_specs=(spec,) * 3, check_vma=False)
```

```python
import functools

import jax
import jax.numpy as jnp
import numpy as np
from jax import lax
from jax.experimental import pallas as pl
from jax.experimental.pallas import tpu as pltpu
from jax.sharding import PartitionSpec as P

MESH = pl.DeviceIdType.MESH
AXES = ("gx", "gy", "gz")
N, B, C = 128, 64, 128
CHUNKS = 8
ROWS = B // CHUNKS
LOG_TOTAL = 27
LINES = (64, 2, 8, 32, 1, 4, 16, 3, 12, 48)


def rev(values, bits):
    values = np.asarray(values)
    return sum(((values >> i) & 1) << (bits - 1 - i) for i in range(bits))


def wave(product, bits):
    angle = 2.0 * np.pi * (product % (1 << bits)) / (1 << bits)
    return np.cos(angle), np.sin(angle)


def np_split(matrix):
    high = np.asarray(matrix, np.float32).astype(jnp.bfloat16)
    low = (np.asarray(matrix, np.float64) - high.astype(np.float64)).astype(jnp.bfloat16)
    return high, low


def tables():
    i = np.arange(N)
    k = rev(i, 7)
    wr, wi = wave(np.outer(k, i), 7)
    mix = np.block([[wr, -wi], [wi, wr]])
    both = lambda pair: np.concatenate(pair, axis=0).astype(np.float32)
    owner = both(wave(np.outer(k, i), 14))
    low_in = both(wave(np.outer(k, i), 27))
    low_out = both(wave(np.outer(k, i), 20))
    e = np.arange(8)
    steps = np.zeros((2 * N, C), np.float32)
    for at, bits in ((0, 20), (32, 13)):
        steps[:, at : at + 8] = both(wave(np.outer(k, e), bits))
        steps[:, at + 8 : at + 16] = both(wave(np.outer(k, 8 * e), bits))
    j = np.arange(8)
    middle = [both(wave(np.outer(j, 128 * chunk + i), 13)) for chunk in range(CHUNKS)]
    turn = both(wave(np.outer(j, i), 10))
    cr, ci = wave(np.outer(i, k), 7)
    scale = 2.0 ** (-LOG_TOTAL / 2)
    last = np.block([[cr, ci], [-ci, cr]]) * scale
    return dict(
        mix=np_split(mix), owner=owner, low_in=low_in, low_out=low_out, steps=steps,
        middle=np.stack(middle), turn=turn, last=np_split(last),
    )


def place():
    gx, gy, gz = (lax.axis_index(a) for a in AXES)
    return gz % 4, (gz // 4) % 4, (gz // 16) * 2 + gx, gy


def halves(x):
    high = x.astype(jnp.bfloat16)
    return high, (x - high.astype(jnp.float32)).astype(jnp.bfloat16)


def dot(a, b):
    return jnp.dot(a, b, preferred_element_type=jnp.float32)


def eight(v):
    def add(p, q):
        return p[0] + q[0], p[1] + q[1]

    def sub(p, q):
        return p[0] - q[0], p[1] - q[1]

    def turn(p):
        return -p[1], p[0]

    def four(p):
        s, d, t, u = add(p[0], p[2]), sub(p[0], p[2]), add(p[1], p[3]), turn(sub(p[1], p[3]))
        return add(s, t), add(d, u), sub(s, t), sub(d, u)

    root = 0.5**0.5
    even, odd = four(v[0::2]), four(v[1::2])
    r, i = odd[1]
    one = ((r - i) * root, (r + i) * root)
    r, i = odd[3]
    three = ((r + i) * -root, (r - i) * root)
    odd = (odd[0], one, turn(odd[2]), three)
    return [add(even[k], odd[k]) for k in range(4)] + [sub(even[k], odd[k]) for k in range(4)]


def times(p, q):
    return p[0] * q[0] - p[1] * q[1], p[0] * q[1] + p[1] * q[0]


def exchange_kernel(
    in_re, in_im, mix_hi, mix_lo, owner, low_in, low_out, steps, middle, out,
    got, sent, back, work, turn_t, w_hi, w_lo, own_t, in_t, out_t, step_t, middle_t, in_fine, in_coarse, out_fine, out_coarse,
    send_sem, own_sem, table_sem, first_sem, second_sem, enter_sem,
):
    x, y, z, core = place()
    me = (z % 2) * 64 + core * 32 + (z // 2) * 16 + y * 4 + x

    def partner(step):
        px = (x + step) % 4
        py = (y + step // 4) % 4
        pz = (z + step // 16) % 4
        pc = (core + step // 64) % 2
        gx, gz = pz % 2, (pz // 2) * 16 + py * 4 + px
        return gx * 64 + pc * 32 + gz, (gx, pc, gz)

    def push(src, dst, sem, device):
        pltpu.make_async_remote_copy(src, dst, send_sem, sem, device_id=device, device_id_type=MESH).start()

    def leg_one(chunk, step):
        d, device = partner(step)
        push(in_re.at[d, :, chunk], got.at[chunk, :, me], first_sem.at[chunk], device)
        push(in_im.at[d, :, chunk], got.at[chunk, :, N + me], first_sem.at[chunk], device)

    def lines(chunks):
        def one(chunk, _):
            for step in LINES:
                leg_one(chunk, step)
            return 0

        lax.fori_loop(*chunks, one, 0)

    def rest(chunk, _):
        def other_core(i, _):
            leg_one(chunk, 65 + i)
            return 0

        def layers(i, _):
            leg_one(chunk, (i // 15 + 1) * 16 + i % 15 + 1)
            return 0

        def plane(i, _):
            leg_one(chunk, (i // 3 + 1) * 4 + i % 3 + 1)
            return 0

        lax.fori_loop(0, 63, other_core, 0)
        lax.fori_loop(0, 45, layers, 0)
        lax.fori_loop(0, 9, plane, 0)
        return 0

    def greet(sem, steps):
        for step in steps:
            pl.semaphore_signal(sem, inc=1, device_id=partner(step)[1], device_id_type=MESH)

    barrier = pltpu.get_barrier_semaphore()
    greet(barrier, LINES)
    pl.semaphore_wait(barrier, len(LINES))
    greet(enter_sem.at[0], (1, 2, 3))
    lines((0, 2))
    pl.semaphore_wait(enter_sem.at[0], 3)
    greet(enter_sem.at[1], (16, 32, 48))
    lines((2, 4))
    pl.semaphore_wait(enter_sem.at[1], 3)
    greet(enter_sem.at[2], (64,))
    lines((4, 8))
    pl.semaphore_wait(enter_sem.at[2], 1)
    lax.fori_loop(0, CHUNKS, rest, 0)

    own = [
        pltpu.make_async_copy(src.at[me, :, chunk], got.at[chunk, :, at + me], own_sem)
        for src, at in ((in_re, 0), (in_im, N))
        for chunk in range(CHUNKS)
    ]
    loads = [
        pltpu.make_async_copy(src, dst, table_sem.at[n])
        for n, (src, dst) in enumerate(
            (
                (mix_hi, w_hi), (mix_lo, w_lo), (owner, own_t), (low_in, in_t), (low_out, out_t), (steps, step_t),
                (middle, middle_t),
            )
        )
    ]
    for copy in own + loads:
        copy.start()
    for copy in loads:
        copy.wait()

    def spread(column):
        return jnp.broadcast_to(column, (N, C))

    lane = lax.broadcasted_iota(jnp.int32, (N, C), 1)
    mine = [jnp.sum(jnp.where(lane == me, own_t[at : at + N], 0.0), axis=1, keepdims=True) for at in (0, N)]
    for low, fine, coarse, at, extra in ((in_t, in_fine, in_coarse, 0, mine), (out_t, out_fine, out_coarse, 32, None)):
        value = low[:N], low[N:]
        if extra is not None:
            value = times(value, (spread(extra[0]), spread(extra[1])))
        for e in range(8):
            step = spread(step_t[:N, at + e : at + e + 1]), spread(step_t[N:, at + e : at + e + 1])
            fine[e, :N], fine[e, N:] = times(value, step)
            coarse[e, :N] = spread(step_t[:N, at + 8 + e : at + 9 + e])
            coarse[e, N:] = spread(step_t[N:, at + 8 + e : at + 9 + e])

    def prepare(chunk, fine, coarse):
        def one(b, _):
            turn_t[b, :N], turn_t[b, N:] = times((fine[chunk, :N], fine[chunk, N:]), (coarse[b, :N], coarse[b, N:]))
            return 0

        lax.fori_loop(0, ROWS, one, 0)

    def transform(src, dst):
        for q in range(ROWS // 2):
            hi, lo = halves(jnp.concatenate([src[2 * q], src[2 * q + 1]], axis=1))
            mixed = dot(w_hi[...], hi) + dot(w_hi[...], lo) + dot(w_lo[...], hi)
            for h in range(2):
                b = 2 * q + h
                part = mixed[:, h * C : (h + 1) * C]
                dst[b, :N], dst[b, N:] = times((part[:N], part[N:]), (turn_t[b, :N], turn_t[b, N:]))

    for _ in range(2):
        pltpu.make_async_copy(in_re.at[0], in_re.at[0], own_sem).wait()

    def there(chunk, _):
        prepare(chunk, in_fine, in_coarse)
        taken = got.at[chunk, :, pl.ds(0, 254)]
        pltpu.make_async_copy(taken, taken, first_sem.at[chunk]).wait()
        transform(got.at[chunk], sent.at[chunk])

        def leg_two(i, _):
            d, device = partner(i + 1)
            push(sent.at[chunk, :, d], back.at[chunk, :, me], second_sem.at[chunk], device)
            push(sent.at[chunk, :, N + d], back.at[chunk, :, N + me], second_sem.at[chunk], device)
            return 0

        lax.fori_loop(0, 127, leg_two, 0)
        for at in (0, N):
            back[chunk, :, pl.ds(at + me, 1), :] = sent[chunk, :, pl.ds(at + me, 1), :]
        return 0

    lax.fori_loop(0, CHUNKS, there, 0)

    def home(chunk, _):
        prepare(chunk, out_fine, out_coarse)
        taken = back.at[chunk, :, pl.ds(0, 254)]
        pltpu.make_async_copy(taken, taken, second_sem.at[chunk]).wait()
        transform(back.at[chunk], work)

        def butterfly(r, _):
            re, im = pl.ds(pl.multiple_of(r * 8, 8), 8), pl.ds(pl.multiple_of(N + r * 8, 8), 8)
            for k, value in enumerate(eight([(work[b, re], work[b, im]) for b in range(8)])):
                turn = middle_t[chunk, k : k + 1], middle_t[chunk, 8 + k : 9 + k]
                out[chunk, k, re], out[chunk, k, im] = times(value, turn)
            return 0

        lax.fori_loop(0, N // 8, butterfly, 0)
        return 0

    lax.fori_loop(0, CHUNKS, home, 0)
    for _ in range(4):
        for chunk in range(CHUNKS):
            moved = got.at[chunk, :, pl.ds(0, 127)]
            pltpu.make_async_copy(moved, moved, send_sem).wait()


GROUP = 16
SEND = 64


def finish_kernel(z, turn, last_hi, last_lo, out_re, out_im, prob, stage, out_sem):
    outs = (out_re, out_im, prob)
    for k in range(8):
        for g in range(N // GROUP):
            re, im = slice(g * GROUP, (g + 1) * GROUP), slice(N + g * GROUP, N + (g + 1) * GROUP)
            high, low = [], []
            for n, value in enumerate(eight([(z[b, k, re], z[b, k, im]) for b in range(8)])):
                parts = [halves(v) for v in times(value, (turn[n : n + 1], turn[8 + n : 9 + n]))]
                high.append(jnp.concatenate([p[0] for p in parts], axis=1))
                low.append(jnp.concatenate([p[1] for p in parts], axis=1))
            high, low = jnp.concatenate(high, axis=0), jnp.concatenate(low, axis=0)
            result = dot(high, last_hi[...]) + dot(low, last_hi[...]) + dot(high, last_lo[...])
            for n in range(8):
                r, i = result[n * GROUP : (n + 1) * GROUP, :C], result[n * GROUP : (n + 1) * GROUP, C:]
                for o, value in enumerate((r, i, r * r + i * i)):
                    stage[k, o, n, re] = value
            if (g + 1) * GROUP % SEND == 0:
                rows = slice((g + 1) * GROUP - SEND, (g + 1) * GROUP)
                for o, ref in enumerate(outs):
                    for n in range(8):
                        place_of = int(rev(k + 8 * n, 6))
                        pltpu.make_async_copy(stage.at[k, o, n, rows], ref.at[rows, place_of], out_sem).start()
    pltpu.make_async_copy(stage, stage, out_sem).wait()


def solution(mesh):
    t = tables()
    f32, bf16 = jnp.float32, jnp.bfloat16
    anywhere, near = pl.BlockSpec(memory_space=pl.ANY), pl.BlockSpec(memory_space=pltpu.VMEM)
    far = pl.BlockSpec(memory_space=pltpu.HBM)
    cube = pltpu.VMEM((CHUNKS, ROWS, 2 * N, C), f32)
    table = pltpu.VMEM((2 * N, C), f32)
    fan = pltpu.VMEM((8, 2 * N, C), f32)
    dma = pltpu.SemaphoreType.DMA

    exchange = pl.pallas_call(
        exchange_kernel,
        out_shape=cube,
        in_specs=[far] * 2 + [anywhere] * 7,
        out_specs=near,
        scratch_shapes=[
            cube, cube, cube, fan, fan,
            pltpu.VMEM((2 * N, 2 * N), bf16), pltpu.VMEM((2 * N, 2 * N), bf16),
            table, table, table, table, pltpu.VMEM((CHUNKS, 16, C), f32), fan, fan, fan, fan,
            dma, dma, dma((7,)), dma((CHUNKS,)), dma((CHUNKS,)), pltpu.SemaphoreType.REGULAR((3,)),
        ],
        compiler_params=pltpu.CompilerParams(has_side_effects=True, collective_id=0, vmem_limit_bytes=48 << 20),
    )
    finish = pl.pallas_call(
        finish_kernel,
        out_shape=[jax.ShapeDtypeStruct((N, B, C), f32)] * 3,
        in_specs=[near] * 4,
        out_specs=[far] * 3,
        scratch_shapes=[pltpu.VMEM((8, 3, 8, N, C), f32), dma],
        compiler_params=pltpu.CompilerParams(vmem_limit_bytes=20 << 20),
    )

    def on_device(state_re, state_im):
        cut = (N, 8, 8, C)
        states = [pltpu.with_memory_space_constraint(s.reshape(cut), pltpu.HBM) for s in (state_re, state_im)]
        names = ("owner", "low_in", "low_out", "steps", "middle")
        z = exchange(*states, *map(jnp.asarray, t["mix"]), *(jnp.asarray(t[name]) for name in names))
        z = pltpu.with_memory_space_constraint(z, pltpu.VMEM)
        outs = finish(z, jnp.asarray(t["turn"]), *map(jnp.asarray, t["last"]))
        return tuple(o.reshape(N * B * C) for o in outs)

    spec = P(AXES)
    return jax.shard_map(on_device, mesh=mesh, in_specs=(spec, spec), out_specs=(spec,) * 3, check_vma=False)
```

```python
import functools

import jax
import jax.numpy as jnp
import numpy as np
from jax import lax
from jax.experimental import pallas as pl
from jax.experimental.pallas import tpu as pltpu
from jax.sharding import PartitionSpec as P

MESH = pl.DeviceIdType.MESH
AXES = ("gx", "gy", "gz")
N, B, C = 128, 64, 128
CHUNKS = 8
ROWS = B // CHUNKS
LOG_TOTAL = 27
LINES = (64, 2, 8, 32, 1, 4, 16, 3, 12, 48)


def rev(values, bits):
    values = np.asarray(values)
    return sum(((values >> i) & 1) << (bits - 1 - i) for i in range(bits))


def wave(product, bits):
    angle = 2.0 * np.pi * (product % (1 << bits)) / (1 << bits)
    return np.cos(angle), np.sin(angle)


def np_split(matrix):
    high = np.asarray(matrix, np.float32).astype(jnp.bfloat16)
    low = (np.asarray(matrix, np.float64) - high.astype(np.float64)).astype(jnp.bfloat16)
    return high, low


def tables():
    i = np.arange(N)
    k = rev(i, 7)
    wr, wi = wave(np.outer(k, i), 7)
    mix = np.block([[wr, -wi], [wi, wr]])
    both = lambda pair: np.concatenate(pair, axis=0).astype(np.float32)
    owner = both(wave(np.outer(k, i), 14))
    low_in = both(wave(np.outer(k, i), 27))
    low_out = both(wave(np.outer(k, i), 20))
    e = np.arange(8)
    steps = np.zeros((2 * N, C), np.float32)
    for at, bits in ((0, 20), (32, 13)):
        steps[:, at : at + 8] = both(wave(np.outer(k, e), bits))
        steps[:, at + 8 : at + 16] = both(wave(np.outer(k, 8 * e), bits))
    j = np.arange(8)
    middle = [both(wave(np.outer(j, 128 * chunk + i), 13)) for chunk in range(CHUNKS)]
    turn = both(wave(np.outer(j, i), 10))
    cr, ci = wave(np.outer(i, k), 7)
    scale = 2.0 ** (-LOG_TOTAL / 2)
    last = np.block([[cr, ci], [-ci, cr]]) * scale
    return dict(
        mix=np_split(mix), owner=owner, low_in=low_in, low_out=low_out, steps=steps,
        middle=np.stack(middle), turn=turn, last=np_split(last),
    )


def place():
    gx, gy, gz = (lax.axis_index(a) for a in AXES)
    return gz % 4, (gz // 4) % 4, (gz // 16) * 2 + gx, gy


def halves(x):
    high = x.astype(jnp.bfloat16)
    return high, (x - high.astype(jnp.float32)).astype(jnp.bfloat16)


def dot(a, b):
    return jnp.dot(a, b, preferred_element_type=jnp.float32)


def eight(v):
    def add(p, q):
        return p[0] + q[0], p[1] + q[1]

    def sub(p, q):
        return p[0] - q[0], p[1] - q[1]

    def turn(p):
        return -p[1], p[0]

    def four(p):
        s, d, t, u = add(p[0], p[2]), sub(p[0], p[2]), add(p[1], p[3]), turn(sub(p[1], p[3]))
        return add(s, t), add(d, u), sub(s, t), sub(d, u)

    root = 0.5**0.5
    even, odd = four(v[0::2]), four(v[1::2])
    r, i = odd[1]
    one = ((r - i) * root, (r + i) * root)
    r, i = odd[3]
    three = ((r + i) * -root, (r - i) * root)
    odd = (odd[0], one, turn(odd[2]), three)
    return [add(even[k], odd[k]) for k in range(4)] + [sub(even[k], odd[k]) for k in range(4)]


def times(p, q):
    return p[0] * q[0] - p[1] * q[1], p[0] * q[1] + p[1] * q[0]


def exchange_kernel(
    in_re, in_im, mix_hi, mix_lo, owner, low_in, low_out, steps, middle, out,
    got, sent, back, work, turn_t, w_hi, w_lo, own_t, in_t, out_t, step_t, middle_t, in_fine, in_coarse, out_fine, out_coarse,
    send_sem, own_sem, table_sem, first_sem, second_sem, enter_sem,
):
    x, y, z, core = place()
    me = (z % 2) * 64 + core * 32 + (z // 2) * 16 + y * 4 + x

    def partner(step):
        px = (x + step) % 4
        py = (y + step // 4) % 4
        pz = (z + step // 16) % 4
        pc = (core + step // 64) % 2
        gx, gz = pz % 2, (pz // 2) * 16 + py * 4 + px
        return gx * 64 + pc * 32 + gz, (gx, pc, gz)

    def push(src, dst, sem, device):
        pltpu.make_async_remote_copy(src, dst, send_sem, sem, device_id=device, device_id_type=MESH).start()

    def leg_one(chunk, step):
        d, device = partner(step)
        push(in_re.at[d, :, chunk], got.at[chunk, :, me], first_sem.at[chunk], device)
        push(in_im.at[d, :, chunk], got.at[chunk, :, N + me], first_sem.at[chunk], device)

    def lines(chunks):
        def one(chunk, _):
            for step in LINES:
                leg_one(chunk, step)
            return 0

        lax.fori_loop(*chunks, one, 0)

    def row(y_step, z_step, core_step):
        py, pz, pc = (y + y_step) % 4, (z + z_step) % 4, (core + core_step) % 2
        gx, gz = pz % 2, (pz // 2) * 16 + py * 4
        return [(gx * 64 + pc * 32 + gz + px, (gx, pc, gz + px)) for px in xs]

    xs = [(x + step) % 4 for step in range(4)]

    def first_leg(chunk, targets):
        for d, device in targets:
            push(in_re.at[d, :, chunk], got.at[chunk, :, me], first_sem.at[chunk], device)
            push(in_im.at[d, :, chunk], got.at[chunk, :, N + me], first_sem.at[chunk], device)

    def rest(chunk, _):
        first_leg(chunk, row(0, 0, 1)[1:])

        def other_core(i, _):
            first_leg(chunk, row(i % 4, i // 4, 1))
            return 0

        def planes(i, _):
            first_leg(chunk, row((i + 1) * (1 - i // 3), (i - 2) * (i // 3), 0)[1:])
            return 0

        def layers(i, _):
            first_leg(chunk, row(i % 3 + 1, i // 3 + 1, 0))
            return 0

        lax.fori_loop(1, 16, other_core, 0)
        lax.fori_loop(0, 6, planes, 0)
        lax.fori_loop(0, 9, layers, 0)
        return 0

    def greet(sem, steps):
        for step in steps:
            pl.semaphore_signal(sem, inc=1, device_id=partner(step)[1], device_id_type=MESH)

    barrier = pltpu.get_barrier_semaphore()
    greet(barrier, LINES)
    pl.semaphore_wait(barrier, len(LINES))
    greet(enter_sem.at[0], (1, 2, 3))
    lines((0, 2))
    pl.semaphore_wait(enter_sem.at[0], 3)
    greet(enter_sem.at[1], (16, 32, 48))
    lines((2, 4))
    pl.semaphore_wait(enter_sem.at[1], 3)
    greet(enter_sem.at[2], (64,))
    lines((4, 8))
    pl.semaphore_wait(enter_sem.at[2], 1)
    lax.fori_loop(0, CHUNKS, rest, 0)

    own = [
        pltpu.make_async_copy(src.at[me, :, chunk], got.at[chunk, :, at + me], own_sem)
        for src, at in ((in_re, 0), (in_im, N))
        for chunk in range(CHUNKS)
    ]
    loads = [
        pltpu.make_async_copy(src, dst, table_sem.at[n])
        for n, (src, dst) in enumerate(
            (
                (mix_hi, w_hi), (mix_lo, w_lo), (owner, own_t), (low_in, in_t), (low_out, out_t), (steps, step_t),
                (middle, middle_t),
            )
        )
    ]
    for copy in own + loads:
        copy.start()
    for copy in loads:
        copy.wait()

    def spread(column):
        return jnp.broadcast_to(column, (N, C))

    lane = lax.broadcasted_iota(jnp.int32, (N, C), 1)
    mine = [jnp.sum(jnp.where(lane == me, own_t[at : at + N], 0.0), axis=1, keepdims=True) for at in (0, N)]
    for low, fine, coarse, at, extra in ((in_t, in_fine, in_coarse, 0, mine), (out_t, out_fine, out_coarse, 32, None)):
        value = low[:N], low[N:]
        if extra is not None:
            value = times(value, (spread(extra[0]), spread(extra[1])))
        for e in range(8):
            step = spread(step_t[:N, at + e : at + e + 1]), spread(step_t[N:, at + e : at + e + 1])
            fine[e, :N], fine[e, N:] = times(value, step)
            coarse[e, :N] = spread(step_t[:N, at + 8 + e : at + 9 + e])
            coarse[e, N:] = spread(step_t[N:, at + 8 + e : at + 9 + e])

    def prepare(chunk, fine, coarse):
        def one(b, _):
            turn_t[b, :N], turn_t[b, N:] = times((fine[chunk, :N], fine[chunk, N:]), (coarse[b, :N], coarse[b, N:]))
            return 0

        lax.fori_loop(0, ROWS, one, 0)

    def transform(src, dst):
        for q in range(ROWS // 2):
            hi, lo = halves(jnp.concatenate([src[2 * q], src[2 * q + 1]], axis=1))
            mixed = dot(w_hi[...], hi) + dot(w_hi[...], lo) + dot(w_lo[...], hi)
            for h in range(2):
                b = 2 * q + h
                part = mixed[:, h * C : (h + 1) * C]
                dst[b, :N], dst[b, N:] = times((part[:N], part[N:]), (turn_t[b, :N], turn_t[b, N:]))

    for _ in range(2):
        pltpu.make_async_copy(in_re.at[0], in_re.at[0], own_sem).wait()

    def there(chunk, _):
        prepare(chunk, in_fine, in_coarse)
        taken = got.at[chunk, :, pl.ds(0, 254)]
        pltpu.make_async_copy(taken, taken, first_sem.at[chunk]).wait()
        transform(got.at[chunk], sent.at[chunk])

        def second_leg(targets):
            for d, device in targets:
                push(sent.at[chunk, :, d], back.at[chunk, :, me], second_sem.at[chunk], device)
                push(sent.at[chunk, :, N + d], back.at[chunk, :, N + me], second_sem.at[chunk], device)

        def corners(i, _):
            second_leg(row(i % 3 + 1, i // 3 % 3 + 1, i // 9)[1:])
            return 0

        def sides(i, _):
            second_leg(row(i % 3 + 1, i // 3 % 3 + 1, i // 9)[:1])
            return 0

        def near_row(i):
            return row((i % 6 + 1) * (1 - i % 6 // 3), (i % 6 - 2) * (i % 6 // 3), i // 6)

        def planes(i, _):
            second_leg(near_row(i)[1:])
            return 0

        def lines_last(i, _):
            second_leg(near_row(i)[:1])
            return 0

        lax.fori_loop(0, 18, corners, 0)
        lax.fori_loop(0, 12, planes, 0)
        lax.fori_loop(0, 18, sides, 0)
        lax.fori_loop(0, 12, lines_last, 0)
        second_leg(row(0, 0, 0)[1:] + row(0, 0, 1)[1:] + row(0, 0, 1)[:1])
        for at in (0, N):
            back[chunk, :, pl.ds(at + me, 1), :] = sent[chunk, :, pl.ds(at + me, 1), :]
        return 0

    lax.fori_loop(0, CHUNKS, there, 0)

    def home(chunk, _):
        prepare(chunk, out_fine, out_coarse)
        taken = back.at[chunk, :, pl.ds(0, 254)]
        pltpu.make_async_copy(taken, taken, second_sem.at[chunk]).wait()
        transform(back.at[chunk], work)

        def butterfly(r, _):
            for at in range(0, 32, 8):
                re, im = pl.ds(pl.multiple_of(r * 32 + at, 8), 8), pl.ds(pl.multiple_of(N + r * 32 + at, 8), 8)
                for k, value in enumerate(eight([(work[b, re], work[b, im]) for b in range(8)])):
                    turn = middle_t[chunk, k : k + 1], middle_t[chunk, 8 + k : 9 + k]
                    out[chunk, k, re], out[chunk, k, im] = times(value, turn)
            return 0

        lax.fori_loop(0, N // 32, butterfly, 0)
        return 0

    lax.fori_loop(0, CHUNKS, home, 0)
    for _ in range(4):
        moved = got.at[:, :, pl.ds(0, 127)]
        pltpu.make_async_copy(moved, moved, send_sem).wait()


GROUP = 16
SEND = 64


def finish_kernel(z, turn, last_hi, last_lo, out_re, out_im, prob, stage, out_sem):
    outs = (out_re, out_im, prob)
    for k in range(8):
        for g in range(N // GROUP):
            re, im = slice(g * GROUP, (g + 1) * GROUP), slice(N + g * GROUP, N + (g + 1) * GROUP)
            high, low = [], []
            for n, value in enumerate(eight([(z[b, k, re], z[b, k, im]) for b in range(8)])):
                parts = [halves(v) for v in times(value, (turn[n : n + 1], turn[8 + n : 9 + n]))]
                high.append(jnp.concatenate([p[0] for p in parts], axis=1))
                low.append(jnp.concatenate([p[1] for p in parts], axis=1))
            high, low = jnp.concatenate(high, axis=0), jnp.concatenate(low, axis=0)
            result = dot(high, last_hi[...]) + dot(low, last_hi[...]) + dot(high, last_lo[...])
            for n in range(8):
                r, i = result[n * GROUP : (n + 1) * GROUP, :C], result[n * GROUP : (n + 1) * GROUP, C:]
                for o, value in enumerate((r, i, r * r + i * i)):
                    stage[k, o, n, re] = value
            if (g + 1) * GROUP % SEND == 0:
                rows = slice((g + 1) * GROUP - SEND, (g + 1) * GROUP)
                for o, ref in enumerate(outs):
                    for n in range(8):
                        place_of = int(rev(k + 8 * n, 6))
                        pltpu.make_async_copy(stage.at[k, o, n, rows], ref.at[rows, place_of], out_sem).start()
    pltpu.make_async_copy(stage, stage, out_sem).wait()


def solution(mesh):
    t = tables()
    f32, bf16 = jnp.float32, jnp.bfloat16
    anywhere, near = pl.BlockSpec(memory_space=pl.ANY), pl.BlockSpec(memory_space=pltpu.VMEM)
    far = pl.BlockSpec(memory_space=pltpu.HBM)
    cube = pltpu.VMEM((CHUNKS, ROWS, 2 * N, C), f32)
    table = pltpu.VMEM((2 * N, C), f32)
    fan = pltpu.VMEM((8, 2 * N, C), f32)
    dma = pltpu.SemaphoreType.DMA

    exchange = pl.pallas_call(
        exchange_kernel,
        out_shape=cube,
        in_specs=[far] * 2 + [anywhere] * 7,
        out_specs=near,
        scratch_shapes=[
            cube, cube, cube, fan, fan,
            pltpu.VMEM((2 * N, 2 * N), bf16), pltpu.VMEM((2 * N, 2 * N), bf16),
            table, table, table, table, pltpu.VMEM((CHUNKS, 16, C), f32), fan, fan, fan, fan,
            dma, dma, dma((7,)), dma((CHUNKS,)), dma((CHUNKS,)), pltpu.SemaphoreType.REGULAR((3,)),
        ],
        compiler_params=pltpu.CompilerParams(has_side_effects=True, collective_id=0, vmem_limit_bytes=48 << 20),
    )
    finish = pl.pallas_call(
        finish_kernel,
        out_shape=[jax.ShapeDtypeStruct((N, B, C), f32)] * 3,
        in_specs=[near] * 4,
        out_specs=[far] * 3,
        scratch_shapes=[pltpu.VMEM((8, 3, 8, N, C), f32), dma],
        compiler_params=pltpu.CompilerParams(vmem_limit_bytes=20 << 20),
    )

    def on_device(state_re, state_im):
        cut = (N, 8, 8, C)
        states = [pltpu.with_memory_space_constraint(s.reshape(cut), pltpu.HBM) for s in (state_re, state_im)]
        names = ("owner", "low_in", "low_out", "steps", "middle")
        z = exchange(*states, *map(jnp.asarray, t["mix"]), *(jnp.asarray(t[name]) for name in names))
        z = pltpu.with_memory_space_constraint(z, pltpu.VMEM)
        outs = finish(z, jnp.asarray(t["turn"]), *map(jnp.asarray, t["last"]))
        return tuple(o.reshape(N * B * C) for o in outs)

    spec = P(AXES)
    return jax.shard_map(on_device, mesh=mesh, in_specs=(spec, spec), out_specs=(spec,) * 3, check_vma=False)
```
